16 devices in a mesh: dp: 2 (over y, z), tp: 8 (over x, core).
Axes of the slice: x: 4, y: 2, z: 1, core: 2. Of those that a mesh axis runs over, the one named last changes fastest.
The devices are a block of a 4x4x8 slice.
Arguments:
- hidden: bfloat16 [16, 584, 1024], P('dp'), parts along dimension 0
- inter_feats: bfloat16 [16, 584, 5, 1024], P('dp'), parts along dimension 0
- proj_grad: bfloat16 [16, 577, 4096], P('dp'), parts along dimension 0
- w_query: bfloat16 [1024, 16, 64], P(None, 'tp')
- w_key: bfloat16 [1024, 16, 64], P(None, 'tp')
- w_value: bfloat16 [1024, 16, 64], P(None, 'tp')
- w_out: bfloat16 [16, 64, 1024], P('tp')
- ln_params: float32 [4, 1024], replicated
- gate_params: float32 [2], replicated
- w_fc1: bfloat16 [1024, 4096], P(None, 'tp')
- b_fc1: float32 [4096], P('tp')
- w_fc2: bfloat16 [4096, 1024], P('tp')
- b_fc2: float32 [1024], replicated
- w_proj: bfloat16 [6144, 4096], P('tp')
- b_proj: float32 [4096], replicated
Outputs:
- output 1: bfloat16 [16, 577, 4096], P(('dp', 'tp')), parts along dimension 0
- output 2: bfloat16 [16, 584, 1024], P('dp'), parts along dimension 0
- output 3: bfloat16 [16, 584, 5, 1024], P('dp'), parts along dimension 0
- output 4: float32 [2048, 16, 64], P('dp', 'tp'), parts along dimension 0
- output 5: float32 [2048, 16, 64], P('dp', 'tp'), parts along dimension 0
- output 6: float32 [2048, 16, 64], P('dp', 'tp'), parts along dimension 0
- output 7: float32 [32, 64, 1024], P(('dp', 'tp')), parts along dimension 0
- output 8: float32 [8, 1024], P('dp'), parts along dimension 0
- output 9: float32 [4], P('dp'), parts along dimension 0
- output 10: float32 [2048, 4096], P('dp', 'tp'), parts along dimension 0
- output 11: float32 [8192], P(('dp', 'tp')), parts along dimension 0
- output 12: float32 [8192, 1024], P(('dp', 'tp')), parts along dimension 0
- output 13: float32 [2048], P('dp'), parts along dimension 0
- output 14: float32 [12288, 4096], P(('dp', 'tp')), parts along dimension 0
- output 15: float32 [8192], P('dp'), parts along dimension 0
There are 2 independent parts. The reference program is written for one: setup_inputs(seed, part) draws one part's arguments, and reference() takes and returns one part's arrays. A program takes and returns all parts, laid end to end along the dimension named above; an argument that names none is the same for every part.
All inputs are finite; a program needn't handle non-finite values.
Results may differ from the reference program's by a relative error of at most 0.0185521.
Values are sent between devices in bfloat16 or wider.
A program may use at most 768 MiB of HBM per device.

```python
import jax
import jax.numpy as jnp
from jax import lax

D = 1024
HEADS = 16
FF = 4096
PROJ_DIM = 4096
NPATCH = 24
NINTER = 5
N_TILES = 8

REAL_TOK = NPATCH * NPATCH + 1
PAD_TOK = (REAL_TOK + 7) // 8 * 8
HEAD_DIM = D // HEADS
FEAT_DIM = (NINTER + 1) * D
LN_EPS = 1e-5


def setup_inputs(seed: int = 0, part: int = 0) -> dict:
    part_keys = jax.random.split(jax.random.fold_in(jax.random.key(seed), part), 4)
    weight_keys = jax.random.split(jax.random.key(seed + 1), 12)

    def normal_draw(slot_id, dims_in, spread):
        return jax.random.normal(weight_keys[slot_id], dims_in, jnp.float32) * spread

    row_scale = jnp.where(jnp.arange(PAD_TOK) < REAL_TOK, 1.0, 30.0)[None, :, None]
    tile_mean = jax.random.normal(part_keys[0], (N_TILES, 1, D), jnp.float32)
    tok_noise = jax.random.normal(part_keys[1], (N_TILES, PAD_TOK, D), jnp.float32)
    hidden = (tile_mean + tok_noise * row_scale).astype(jnp.bfloat16)
    inter_draw = jax.random.normal(part_keys[2], (N_TILES, PAD_TOK, NINTER, D), jnp.float32)
    inter_feats = (inter_draw * row_scale[..., None]).astype(jnp.bfloat16)
    proj_grad = jax.random.normal(part_keys[3], (N_TILES, REAL_TOK, PROJ_DIM), jnp.float32).astype(jnp.bfloat16)
    ln_base = jnp.array([1.0, 0.0, 1.0, 0.0], jnp.float32)[:, None]
    return {
        'hidden': hidden,
        'inter_feats': inter_feats,
        'proj_grad': proj_grad,
        'w_query': normal_draw(0, (D, HEADS, HEAD_DIM), D ** -0.5).astype(jnp.bfloat16),
        'w_key': normal_draw(1, (D, HEADS, HEAD_DIM), D ** -0.5).astype(jnp.bfloat16),
        'w_value': normal_draw(2, (D, HEADS, HEAD_DIM), D ** -0.5).astype(jnp.bfloat16),
        'w_out': normal_draw(3, (HEADS, HEAD_DIM, D), D ** -0.5).astype(jnp.bfloat16),
        'ln_params': ln_base + normal_draw(4, (4, D), 0.3),
        'gate_params': jax.random.uniform(weight_keys[5], (2,), jnp.float32, 0.6, 1.2),
        'w_fc1': normal_draw(6, (D, FF), D ** -0.5).astype(jnp.bfloat16),
        'b_fc1': normal_draw(7, (FF,), 0.5),
        'w_fc2': normal_draw(8, (FF, D), FF ** -0.5).astype(jnp.bfloat16),
        'b_fc2': normal_draw(9, (D,), 0.5),
        'w_proj': normal_draw(10, (FEAT_DIM, PROJ_DIM), FEAT_DIM ** -0.5).astype(jnp.bfloat16),
        'b_proj': normal_draw(11, (PROJ_DIM,), 0.5),
    }


def layer_norm(values, ln_gain, ln_bias):
    row_mean = jnp.mean(values, axis=-1, keepdims=True)
    centred = values - row_mean
    row_var = jnp.mean(centred * centred, axis=-1, keepdims=True)
    return centred * lax.rsqrt(row_var + LN_EPS) * ln_gain + ln_bias


def tile_forward(tile_x, tile_inter, w_query, w_key, w_value, w_out, ln_params, gate_params, w_fc1, b_fc1, w_fc2, b_fc2, w_proj, b_proj):
    x_wide = tile_x.astype(jnp.float32)
    normed = layer_norm(x_wide, ln_params[0], ln_params[1]).astype(jnp.bfloat16)
    q_act = jnp.dot(normed, w_query.reshape(D, D), preferred_element_type=jnp.float32).astype(jnp.bfloat16).reshape(PAD_TOK, HEADS, HEAD_DIM)
    k_act = jnp.dot(normed, w_key.reshape(D, D), preferred_element_type=jnp.float32).astype(jnp.bfloat16).reshape(PAD_TOK, HEADS, HEAD_DIM)
    v_act = jnp.dot(normed, w_value.reshape(D, D), preferred_element_type=jnp.float32).astype(jnp.bfloat16).reshape(PAD_TOK, HEADS, HEAD_DIM)
    scores = jnp.einsum('qhe,khe->hqk', q_act.astype(jnp.float32), k_act.astype(jnp.float32)) * HEAD_DIM ** -0.5
    key_ok = jnp.arange(PAD_TOK) < REAL_TOK
    scores = jnp.where(key_ok[None, None, :], scores, -1e30)
    attn_probs = jax.nn.softmax(scores, axis=-1).astype(jnp.bfloat16)
    context = jnp.einsum('hqk,khe->qhe', attn_probs.astype(jnp.float32), v_act.astype(jnp.float32)).astype(jnp.bfloat16).reshape(PAD_TOK, D)
    attn_out = jnp.dot(context, w_out.reshape(D, D), preferred_element_type=jnp.float32)
    x_one = (x_wide + jnp.tanh(gate_params[0]) * attn_out).astype(jnp.bfloat16)
    x_one_wide = x_one.astype(jnp.float32)
    normed_two = layer_norm(x_one_wide, ln_params[2], ln_params[3]).astype(jnp.bfloat16)
    pre_act = jnp.dot(normed_two, w_fc1, preferred_element_type=jnp.float32) + b_fc1
    mlp_act = jax.nn.gelu(pre_act, approximate=False).astype(jnp.bfloat16)
    mlp_out = jnp.dot(mlp_act, w_fc2, preferred_element_type=jnp.float32) + b_fc2
    x_two = (x_one_wide + jnp.tanh(gate_params[1]) * mlp_out).astype(jnp.bfloat16)
    features = jnp.concatenate([x_two, tile_inter.reshape(PAD_TOK, NINTER * D)], axis=-1)[:REAL_TOK]
    return (jnp.dot(features, w_proj, preferred_element_type=jnp.float32) + b_proj).astype(jnp.bfloat16)


def reference(hidden, inter_feats, proj_grad, w_query, w_key, w_value, w_out, ln_params, gate_params, w_fc1, b_fc1, w_fc2, b_fc2, w_proj, b_proj):
    weights = (w_query, w_key, w_value, w_out, ln_params, gate_params, w_fc1, b_fc1, w_fc2, b_fc2, w_proj, b_proj)

    def tile_step(grad_acc, tile_data):
        tile_x, tile_inter, tile_grad = tile_data
        tile_out, pull_back = jax.vjp(tile_forward, tile_x, tile_inter, w_query, w_key, w_value, w_out, ln_params, gate_params, w_fc1, b_fc1, w_fc2, b_fc2, w_proj, b_proj)
        grad_list = pull_back(tile_grad)
        new_acc = tuple(acc_item + grad_item.astype(jnp.float32) for acc_item, grad_item in zip(grad_acc, grad_list[2:]))
        return new_acc, (tile_out, grad_list[0], grad_list[1])

    zero_grads = tuple(jnp.zeros(weight.shape, jnp.float32) for weight in weights)
    grad_acc, tile_results = lax.scan(tile_step, zero_grads, (hidden, inter_feats, proj_grad))
    proj_out, grad_hidden, grad_inter = tile_results
    return (proj_out, grad_hidden, grad_inter, grad_acc[0], grad_acc[1], grad_acc[2], grad_acc[3], grad_acc[4], grad_acc[5], grad_acc[6], grad_acc[7], grad_acc[8], grad_acc[9], grad_acc[10], grad_acc[11])
```

```python
import functools
import math
import jax
import jax.numpy as jnp
from jax import lax
from jax.experimental import pallas as pl
from jax.experimental.layout import Layout, with_layout_constraint
from jax.experimental.pallas import tpu as pltpu
from jax.sharding import PartitionSpec as P

LN_EPS = 1e-5


def layer_norm(values, ln_gain, ln_bias):
    row_mean = jnp.mean(values, axis=-1, keepdims=True)
    centred = values - row_mean
    row_var = jnp.mean(centred * centred, axis=-1, keepdims=True)
    return (centred * lax.rsqrt(row_var + LN_EPS) * ln_gain + ln_bias).astype(jnp.bfloat16)


def gelu_bf16(pre_act):
    return jax.nn.gelu(pre_act, approximate=False).astype(jnp.bfloat16)


def matmul(eq_form, lhs_in, rhs_in):
    return jnp.einsum(eq_form, lhs_in, rhs_in, preferred_element_type=jnp.float32)


def after(value, earlier):
    return lax.optimization_barrier((value, earlier))


def attend(real_rows, q_act, k_act, v_act):
    tokens = q_act.shape[0]
    score_scale = q_act.shape[2] ** -0.5
    scores = matmul('qhe,khe->hqk', q_act, k_act) * score_scale
    key_ok = (jnp.arange(tokens) < real_rows)[None, None, :]
    attn_probs = jax.nn.softmax(jnp.where(key_ok, scores, -1e30), axis=-1).astype(jnp.bfloat16)
    return matmul('hqk,khe->qhe', attn_probs, v_act).astype(jnp.bfloat16)


def feats_kernel(blocks, piece, real_rows, grad_ref, rows_ref, *rest):
    out_ref, held, sems = rest[-3:]
    tokens = held.shape[2]
    tile = pl.program_id(0)
    tiles = pl.num_programs(0)
    slot = lax.rem(tile, 2)

    def copies(at_tile, at_slot):
        return [pltpu.make_async_copy(held.at[at_slot, n],
                                      out_ref.at[at_tile, feat, :, pl.ds(col * piece, piece)],
                                      sems.at[at_slot, n])
                for n, (_, feat, col) in enumerate(blocks)]

    @pl.when(tile >= 2)
    def _():
        for copy in copies(tile - 2, slot):
            copy.wait()

    is_real = lax.broadcasted_iota(jnp.int32, (tokens, piece), 0) < real_rows
    out_now = copies(tile, slot)
    for n, (row, _, _) in enumerate(blocks):
        block = lax.dot_general(grad_ref[0], rows_ref[pl.ds(row * piece, piece), :],
                                (((1,), (1,)), ((), ())), preferred_element_type=jnp.float32)
        held[slot, n] = jnp.where(is_real, block, 0.0).astype(jnp.bfloat16)
        out_now[n].start()

    @pl.when(tile == tiles - 1)
    def _():
        for copy in copies(tile - 1, 1 - slot) + out_now:
            copy.wait()


def grad_feats_part(grad, rows, blocks, piece, feats, tokens, width, prior):
    tiles, real_rows, depth = grad.shape
    flops = 2 * tiles * tokens * depth * piece * len(blocks)
    in_specs = [pl.BlockSpec((1, tokens, depth), lambda b: (b, 0, 0)),
                pl.BlockSpec(rows.shape, lambda b: (0, 0), pipeline_mode=pl.Buffered(1))]
    args = [grad, rows]
    aliases = {}
    if prior is not None:
        in_specs.append(pl.BlockSpec(memory_space=pl.ANY))
        args.append(prior)
        aliases = {2: 0}
    return pl.pallas_call(
        functools.partial(feats_kernel, blocks, piece, real_rows),
        grid=(tiles,),
        out_shape=jax.ShapeDtypeStruct((tiles, feats, tokens, width), jnp.bfloat16),
        in_specs=in_specs,
        out_specs=pl.BlockSpec(memory_space=pl.ANY),
        scratch_shapes=[pltpu.VMEM((2, len(blocks), tokens, piece), jnp.bfloat16),
                        pltpu.SemaphoreType.DMA((2, len(blocks)))],
        input_output_aliases=aliases,
        compiler_params=pltpu.CompilerParams(dimension_semantics=("arbitrary",), vmem_limit_bytes=58 * 1024 * 1024),
        cost_estimate=pl.CostEstimate(flops=flops, bytes_accessed=2 * (grad.size + rows.size + tiles * tokens * piece * len(blocks)), transcendentals=0),
    )(*args)


def rows_grad_kernel(real_rows, step, feats_ref, grad_ref, out_ref):
    tile = pl.program_id(0)
    tokens, depth = grad_ref.shape[1:]

    @pl.when(tile == 0)
    def _():
        out_ref[...] = jnp.zeros_like(out_ref)

    is_real = lax.broadcasted_iota(jnp.int32, (tokens, step), 0) < real_rows
    turned = feats_ref[0].T
    for at in range(0, depth, step):
        cols = pl.ds(at, step)
        grad = jnp.where(is_real, grad_ref[0, :, cols], jnp.bfloat16(0))
        out_ref[:, cols] += jnp.dot(turned, grad, preferred_element_type=jnp.float32)


def rows_grad(feats_local, grad):
    tiles, tokens, local = feats_local.shape
    real_rows, depth = grad.shape[1:]
    return pl.pallas_call(
        functools.partial(rows_grad_kernel, real_rows, min(512, depth)),
        grid=(tiles,),
        out_shape=jax.ShapeDtypeStruct((local, depth), jnp.float32),
        in_specs=[pl.BlockSpec((1, tokens, local), lambda b: (b, 0, 0)),
                  pl.BlockSpec((1, tokens, depth), lambda b: (b, 0, 0))],
        out_specs=pl.BlockSpec((local, depth), lambda b: (0, 0)),
        compiler_params=pltpu.CompilerParams(dimension_semantics=("arbitrary",), vmem_limit_bytes=58 * 1024 * 1024),
        cost_estimate=pl.CostEstimate(flops=2 * tiles * tokens * local * depth, bytes_accessed=2 * (feats_local.size + grad.size) + 4 * local * depth, transcendentals=0),
    )(feats_local, grad)


def local_step(hidden, inter_feats, proj_grad, w_query, w_key, w_value, w_out, ln_params, gate_params, w_fc1, b_fc1, w_fc2, b_fc2, w_proj, b_proj):
    tile_count, tokens, width = hidden.shape
    real_rows = proj_grad.shape[1]
    feats = inter_feats.shape[2]
    feat_local, proj_dim = w_proj.shape
    local_heads, head_dim = w_query.shape[1:]
    local_width = local_heads * head_dim
    group = lax.axis_size('tp')
    heads = group * local_heads
    mine = lax.axis_index('tp')
    piece = math.gcd(feat_local, width)
    per_dev, per_feat = feat_local // piece, width // piece

    flip = lambda w: w.reshape(width, local_width).T
    w_attn = lax.all_gather(jnp.stack([flip(w_query), flip(w_key), flip(w_value), w_out.reshape(local_width, width)]), 'tp', axis=1, tiled=True)
    fc1 = lax.all_gather(w_fc1, 'tp', axis=1, tiled=True)
    bias1 = lax.all_gather(b_fc1, 'tp', axis=0, tiled=True)
    fc2 = lax.all_gather(w_fc2, 'tp', axis=0, tiled=True)
    gather_rows = lambda part: lax.all_gather(part, 'tp', axis=0, tiled=True)
    w_parts = [w_proj[j * piece:(j + 1) * piece] for j in range(per_dev)]

    x_wide = lax.dynamic_index_in_dim(hidden, mine, 0, keepdims=False).astype(jnp.float32)
    normed, norm1_pull = jax.vjp(layer_norm, x_wide, ln_params[0], ln_params[1])
    proj_grad = with_layout_constraint(proj_grad, Layout((0, 1, 2)))
    normed, (proj_grad, w_parts[0]) = after(normed, (proj_grad, w_parts[0]))
    proj_rows = [gather_rows(w_parts[0])]
    w_qkv = w_attn[:3].reshape(3 * width, width)
    qkv = matmul('td,jd->tj', normed, w_qkv).astype(jnp.bfloat16).reshape(tokens, 3, heads, head_dim)
    context, attend_pull = jax.vjp(functools.partial(attend, real_rows), qkv[:, 0], qkv[:, 1], qkv[:, 2])
    context = context.reshape(tokens, width)
    attn_out = matmul('tj,jd->td', context, w_attn[3])
    gate_attn = jnp.tanh(gate_params[0])
    gate_mlp = jnp.tanh(gate_params[1])
    x_one_wide = (x_wide + gate_attn * attn_out).astype(jnp.bfloat16).astype(jnp.float32)
    normed_two, norm2_pull = jax.vjp(layer_norm, x_one_wide, ln_params[2], ln_params[3])
    pre_act = matmul('td,df->tf', normed_two, fc1) + bias1
    mlp_act, gelu_pull = jax.vjp(gelu_bf16, pre_act)
    mlp_out = matmul('tf,fd->td', mlp_act, fc2) + b_fc2
    x_two = (x_one_wide + gate_mlp * mlp_out).astype(jnp.bfloat16)

    inter = jnp.transpose(inter_feats, (0, 2, 1, 3))
    grad_mine = lax.dynamic_index_in_dim(proj_grad, mine, 0, keepdims=False)

    def feats_part(j, prior):
        blocks = []
        for d in range(group):
            at = d * per_dev + j
            if at >= per_feat:
                blocks.append((d, at // per_feat - 1, at % per_feat))
        return grad_feats_part(proj_grad, proj_rows[j], tuple(blocks), piece, feats, tokens, width, prior)

    w_parts[1], x_two = after(w_parts[1], x_two)
    x_two_all = lax.all_gather(x_two, 'tp', axis=0, tiled=False)
    proj_rows.append(gather_rows(w_parts[1]))
    proj_rows[0], x_two = after(proj_rows[0], x_two)
    for part in w_parts[2:]:
        part, proj_rows[0] = after(part, proj_rows[0])
        proj_rows.append(gather_rows(part))
    grad_inter = feats_part(0, None)
    x_two_all, grad_inter = after(x_two_all, grad_inter)

    cols = []
    for j in range(per_dev):
        at = mine * per_dev + j
        feat, col = at // per_feat, (at % per_feat) * piece
        from_two = lax.dynamic_slice_in_dim(x_two_all, col, piece, axis=2)
        from_inter = lax.dynamic_slice(inter, (0, jnp.maximum(feat - 1, 0), 0, col), (tile_count, 1, tokens, piece))[:, 0]
        cols.append(jnp.where(feat == 0, from_two, from_inter))
    feats_local = jnp.concatenate(cols, axis=-1)
    grad_w_proj = rows_grad(feats_local, proj_grad)
    for j in range(1, per_dev - 1):
        proj_rows[j], grad_w_proj = after(proj_rows[j], grad_w_proj)
        grad_inter = feats_part(j, grad_inter)
    proj_rows[-1], grad_inter = after(proj_rows[-1], grad_inter)

    rows_two = jnp.concatenate([proj_rows[at % per_dev][(at // per_dev) * piece:(at // per_dev + 1) * piece] for at in range(per_feat)], axis=0)
    grad_x_two = matmul('tp,cp->tc', grad_mine, rows_two).astype(jnp.bfloat16)
    grad_x_two = jnp.pad(grad_x_two, ((0, tokens - real_rows), (0, 0))).astype(jnp.float32)
    grad_mlp = gate_mlp * grad_x_two
    grad_gate_mlp = jnp.sum(grad_x_two * mlp_out) * (1.0 - gate_mlp * gate_mlp)
    grad_b_fc2 = jnp.sum(grad_mlp, axis=0)
    grad_mlp_low = grad_mlp.astype(jnp.bfloat16)
    grad_fc2 = matmul('tf,td->fd', mlp_act, grad_mlp_low).astype(jnp.bfloat16)
    grad_act = matmul('td,fd->tf', grad_mlp_low, fc2).astype(jnp.bfloat16)
    grad_pre = gelu_pull(grad_act)[0]
    grad_b_fc1 = jnp.sum(grad_pre, axis=0)
    grad_pre_low = grad_pre.astype(jnp.bfloat16)
    grad_fc1 = matmul('tf,td->fd', grad_pre_low, normed_two).astype(jnp.bfloat16)
    grad_normed_two = matmul('tf,df->td', grad_pre_low, fc1).astype(jnp.bfloat16)
    grad_normed_two, (grad_fc1, grad_fc2) = after(grad_normed_two, (grad_fc1, grad_fc2))
    grad_w_fc2 = lax.psum_scatter(grad_fc2, 'tp', scatter_dimension=0, tiled=True)
    grad_w_fc1 = lax.psum_scatter(grad_fc1, 'tp', scatter_dimension=0, tiled=True)
    grad_x_ln_two, grad_gain_two, grad_bias_two = norm2_pull(grad_normed_two)
    grad_x_one = (grad_x_two + grad_x_ln_two).astype(jnp.bfloat16).astype(jnp.float32)
    grad_attn = gate_attn * grad_x_one
    grad_gate_attn = jnp.sum(grad_x_one * attn_out) * (1.0 - gate_attn * gate_attn)
    grad_attn_low = grad_attn.astype(jnp.bfloat16)
    grad_wo = matmul('tj,td->jd', context, grad_attn_low)
    grad_context = matmul('td,jd->tj', grad_attn_low, w_attn[3]).astype(jnp.bfloat16).reshape(tokens, heads, head_dim)
    grad_qkv = jnp.stack(attend_pull(grad_context), axis=1).reshape(tokens, 3 * width)
    grad_wqkv = matmul('tj,td->jd', grad_qkv, normed).reshape(3, width, width)
    grad_w_attn = jnp.concatenate([grad_wqkv, grad_wo[None]]).astype(jnp.bfloat16)
    grad_w_attn = lax.psum_scatter(grad_w_attn, 'tp', scatter_dimension=1, tiled=True).astype(jnp.float32)
    unflip = lambda g: g.T.reshape(width, local_heads, head_dim)
    grad_normed = matmul('tj,jd->td', grad_qkv, w_qkv).astype(jnp.bfloat16)
    grad_x_ln, grad_gain, grad_bias = norm1_pull(grad_normed)
    grad_tile = (grad_x_one + grad_x_ln).astype(jnp.bfloat16)

    proj_rows[-1], grad_tile = after(proj_rows[-1], grad_tile)
    grad_tile, (grad_w_fc1, grad_w_fc2) = after(grad_tile, (grad_w_fc1, grad_w_fc2))
    grad_hidden = lax.all_gather(grad_tile, 'tp', axis=0, tiled=False)
    grad_w_fc1, grad_w_fc2 = grad_w_fc1.astype(jnp.float32).T, grad_w_fc2.astype(jnp.float32)
    grad_inter = jnp.transpose(feats_part(per_dev - 1, grad_inter), (0, 2, 1, 3))
    inter_mine = lax.dynamic_index_in_dim(inter, mine, 0, keepdims=False)
    feats_mine = jnp.concatenate([x_two[None], inter_mine], axis=0)[:, :real_rows]
    proj_sum = b_proj
    for j in range(per_dev):
        part = jnp.concatenate([feats_mine[at // per_feat, :, (at % per_feat) * piece:(at % per_feat + 1) * piece]
                                for at in range(j, group * per_dev, per_dev)], axis=-1)
        proj_sum = proj_sum + matmul('tc,cp->tp', part, proj_rows[j])
    proj_out = proj_sum.astype(jnp.bfloat16)[None]

    grad_b_proj = jnp.sum(grad_mine, axis=0, dtype=jnp.float32)
    small = [grad_gain, grad_bias, grad_gain_two, grad_bias_two, grad_b_fc2, grad_b_fc1, grad_b_proj, jnp.stack([grad_gate_attn, grad_gate_mlp])]
    sums = lax.psum(jnp.concatenate(small), 'tp')
    ends = [sum(s.shape[0] for s in small[:n + 1]) for n in range(len(small))]
    grad_gain, grad_bias, grad_gain_two, grad_bias_two, grad_b_fc2, grad_b_fc1, grad_b_proj, grad_gates = jnp.split(sums, ends[:-1])
    grad_ln = jnp.stack([grad_gain, grad_bias, grad_gain_two, grad_bias_two])
    grad_b_fc1 = lax.dynamic_slice_in_dim(grad_b_fc1, mine * b_fc1.shape[0], b_fc1.shape[0], axis=0)
    return (proj_out, grad_hidden, grad_inter, unflip(grad_w_attn[0]), unflip(grad_w_attn[1]), unflip(grad_w_attn[2]), grad_w_attn[3].reshape(local_heads, head_dim, width), grad_ln, grad_gates, grad_w_fc1, grad_b_fc1, grad_w_fc2, grad_b_fc2, grad_w_proj, grad_b_proj)


def solution(mesh):
    tiles_spec = P('dp', None, None)
    inter_spec = P('dp', None, None, None)
    head_cols = P(None, 'tp', None)
    in_specs = (tiles_spec, inter_spec, tiles_spec, head_cols, head_cols, head_cols, P('tp', None, None), P(None, None), P(None), P(None, 'tp'), P('tp'), P('tp', None), P(None), P('tp', None), P(None))
    grad_heads = P('dp', 'tp', None)
    out_specs = (P(('dp', 'tp'), None, None), tiles_spec, inter_spec, grad_heads, grad_heads, grad_heads, P(('dp', 'tp'), None, None), P('dp', None), P('dp'), P('dp', 'tp'), P(('dp', 'tp')), P(('dp', 'tp'), None), P('dp'), P(('dp', 'tp'), None), P('dp'))
    return jax.shard_map(local_step, mesh=mesh, in_specs=in_specs, out_specs=out_specs, check_vma=False)
```

```python
import functools
import math
import jax
import jax.numpy as jnp
from jax import lax
from jax.experimental import pallas as pl
from jax.experimental.layout import Layout, with_layout_constraint
from jax.experimental.pallas import tpu as pltpu
from jax.sharding import PartitionSpec as P

LN_EPS = 1e-5


def layer_norm(values, ln_gain, ln_bias):
    row_mean = jnp.mean(values, axis=-1, keepdims=True)
    centred = values - row_mean
    row_var = jnp.mean(centred * centred, axis=-1, keepdims=True)
    return (centred * lax.rsqrt(row_var + LN_EPS) * ln_gain + ln_bias).astype(jnp.bfloat16)


def gelu_bf16(pre_act):
    return jax.nn.gelu(pre_act, approximate=False).astype(jnp.bfloat16)


def matmul(eq_form, lhs_in, rhs_in):
    return jnp.einsum(eq_form, lhs_in, rhs_in, preferred_element_type=jnp.float32)


def after(value, earlier):
    return lax.optimization_barrier((value, earlier))


def head_probs(real_rows, q_act, k_pad):
    scores = lax.dot_general(q_act, k_pad, (((1,), (1,)), ((), ())), preferred_element_type=jnp.float32)
    key_ok = lax.broadcasted_iota(jnp.int32, scores.shape, 1) < real_rows
    scores = jnp.where(key_ok, scores * q_act.shape[1] ** -0.5, -1e30)
    raised = jnp.exp(scores - jnp.max(scores, axis=-1, keepdims=True))
    return raised / jnp.sum(raised, axis=-1, keepdims=True)


def pad_keys(pads, refs):
    tokens = refs[0].shape[0]
    for pad_ref, ref in zip(pads, refs):
        pad_ref[0:tokens, :] = ref[...]
        pad_ref[tokens:, :] = jnp.zeros((pad_ref.shape[0] - tokens, pad_ref.shape[1]), pad_ref.dtype)


def attend_kernel(real_rows, head_dim, q_ref, k_ref, v_ref, out_ref, k_pad, v_pad):
    pad_keys((k_pad, v_pad), (k_ref, v_ref))
    for at in range(0, q_ref.shape[1], head_dim):
        cols = slice(at, at + head_dim)
        probs = head_probs(real_rows, q_ref[:, cols], k_pad[:, cols]).astype(jnp.bfloat16)
        out_ref[:, cols] = jnp.dot(probs, v_pad[:, cols], preferred_element_type=jnp.float32).astype(jnp.bfloat16)


def attend_grad_kernel(real_rows, head_dim, q_ref, k_ref, v_ref, grad_ref, out_ref, k_pad, v_pad):
    pad_keys((k_pad, v_pad), (k_ref, v_ref))
    tokens = q_ref.shape[0]
    over_rows = (((0,), (0,)), ((), ()))
    for at in range(0, q_ref.shape[1], head_dim):
        cols = slice(at, at + head_dim)
        q_act, grad = q_ref[:, cols], grad_ref[:, cols]
        probs = head_probs(real_rows, q_act, k_pad[:, cols])
        grad_v = lax.dot_general(probs.astype(jnp.bfloat16), grad, over_rows, preferred_element_type=jnp.float32)
        grad_p = lax.dot_general(grad, v_pad[:, cols], (((1,), (1,)), ((), ())), preferred_element_type=jnp.float32)
        grad_p = grad_p.astype(jnp.bfloat16).astype(jnp.float32)
        centre = jnp.sum(probs * grad_p, axis=-1, keepdims=True)
        grad_s = (probs * (grad_p - centre) * head_dim ** -0.5).astype(jnp.bfloat16)
        grad_k = lax.dot_general(grad_s, q_act, over_rows, preferred_element_type=jnp.float32)
        grad_q = jnp.dot(grad_s, k_pad[:, cols], preferred_element_type=jnp.float32)
        out_ref[0, :, cols] = grad_q.astype(jnp.bfloat16)
        out_ref[1, :, cols] = grad_k[0:tokens].astype(jnp.bfloat16)
        out_ref[2, :, cols] = grad_v[0:tokens].astype(jnp.bfloat16)


def attend(real_rows, head_dim, width, qkv, grad=None):
    tokens = qkv.shape[0]
    lanes = max(128, head_dim)
    steps = width // lanes
    keys = (tokens + 127) // 128 * 128
    part = lambda n: pl.BlockSpec((tokens, lanes), lambda h, n=n: (0, n * steps + h))
    one = 2 * tokens * keys * width
    args, in_specs = [qkv, qkv, qkv], [part(0), part(1), part(2)]
    if grad is None:
        kernel, dots = attend_kernel, 2
        out_shape, out_specs = (tokens, width), part(0)
    else:
        kernel, dots = attend_grad_kernel, 5
        args, in_specs = args + [grad], in_specs + [part(0)]
        out_shape, out_specs = (3, tokens, width), pl.BlockSpec((3, tokens, lanes), lambda h: (0, 0, h))
    return pl.pallas_call(
        functools.partial(kernel, real_rows, head_dim),
        grid=(steps,),
        out_shape=jax.ShapeDtypeStruct(out_shape, jnp.bfloat16),
        in_specs=in_specs,
        out_specs=out_specs,
        scratch_shapes=[pltpu.VMEM((keys, lanes), jnp.bfloat16)] * 2,
        compiler_params=pltpu.CompilerParams(dimension_semantics=("arbitrary",), vmem_limit_bytes=40 * 1024 * 1024),
        cost_estimate=pl.CostEstimate(flops=4 * dots * one, bytes_accessed=16 * tokens * width, transcendentals=0),
    )(*args)


def split_exact(values):
    high = lax.reduce_precision(values, 8, 7)
    mid = lax.reduce_precision(values - high, 8, 7)
    return jnp.stack([high, mid, values - high - mid]).astype(jnp.bfloat16)


def feats_kernel(blocks, piece, real_rows, grad_ref, rows_ref, *rest):
    out_ref, held, sems = rest[-3:]
    tokens = held.shape[2]
    tile = pl.program_id(0)
    tiles = pl.num_programs(0)
    slot = lax.rem(tile, 2)

    def copies(at_tile, at_slot):
        return [pltpu.make_async_copy(held.at[at_slot, n],
                                      out_ref.at[at_tile, feat, :, pl.ds(col * piece, piece)],
                                      sems.at[at_slot, n])
                for n, (_, feat, col) in enumerate(blocks)]

    @pl.when(tile >= 2)
    def _():
        for copy in copies(tile - 2, slot):
            copy.wait()

    is_real = lax.broadcasted_iota(jnp.int32, (tokens, piece), 0) < real_rows
    out_now = copies(tile, slot)
    for n, (row, _, _) in enumerate(blocks):
        block = lax.dot_general(grad_ref[0], rows_ref[pl.ds(row * piece, piece), :],
                                (((1,), (1,)), ((), ())), preferred_element_type=jnp.float32)
        held[slot, n] = jnp.where(is_real, block, 0.0).astype(jnp.bfloat16)
        out_now[n].start()

    @pl.when(tile == tiles - 1)
    def _():
        for copy in copies(tile - 1, 1 - slot) + out_now:
            copy.wait()


def grad_feats_part(grad, rows, blocks, piece, feats, tokens, width, prior):
    tiles, real_rows, depth = grad.shape
    flops = 2 * tiles * tokens * depth * piece * len(blocks)
    in_specs = [pl.BlockSpec((1, tokens, depth), lambda b: (b, 0, 0)),
                pl.BlockSpec(rows.shape, lambda b: (0, 0), pipeline_mode=pl.Buffered(1))]
    args = [grad, rows]
    aliases = {}
    if prior is not None:
        in_specs.append(pl.BlockSpec(memory_space=pl.ANY))
        args.append(prior)
        aliases = {2: 0}
    return pl.pallas_call(
        functools.partial(feats_kernel, blocks, piece, real_rows),
        grid=(tiles,),
        out_shape=jax.ShapeDtypeStruct((tiles, feats, tokens, width), jnp.bfloat16),
        in_specs=in_specs,
        out_specs=pl.BlockSpec(memory_space=pl.ANY),
        scratch_shapes=[pltpu.VMEM((2, len(blocks), tokens, piece), jnp.bfloat16),
                        pltpu.SemaphoreType.DMA((2, len(blocks)))],
        input_output_aliases=aliases,
        compiler_params=pltpu.CompilerParams(dimension_semantics=("arbitrary",), vmem_limit_bytes=58 * 1024 * 1024),
        cost_estimate=pl.CostEstimate(flops=flops, bytes_accessed=2 * (grad.size + rows.size + tiles * tokens * piece * len(blocks)), transcendentals=0),
    )(*args)


def rows_grad_kernel(real_rows, step, feats_ref, grad_ref, out_ref):
    tile = pl.program_id(0)
    tokens, depth = grad_ref.shape[1:]

    @pl.when(tile == 0)
    def _():
        out_ref[...] = jnp.zeros_like(out_ref)

    is_real = lax.broadcasted_iota(jnp.int32, (tokens, step), 0) < real_rows
    turned = feats_ref[0].T
    for at in range(0, depth, step):
        cols = pl.ds(at, step)
        grad = jnp.where(is_real, grad_ref[0, :, cols], jnp.bfloat16(0))
        out_ref[:, cols] += jnp.dot(turned, grad, preferred_element_type=jnp.float32)


def rows_grad(feats_local, grad):
    tiles, tokens, local = feats_local.shape
    real_rows, depth = grad.shape[1:]
    return pl.pallas_call(
        functools.partial(rows_grad_kernel, real_rows, min(512, depth)),
        grid=(tiles,),
        out_shape=jax.ShapeDtypeStruct((local, depth), jnp.float32),
        in_specs=[pl.BlockSpec((1, tokens, local), lambda b: (b, 0, 0)),
                  pl.BlockSpec((1, tokens, depth), lambda b: (b, 0, 0))],
        out_specs=pl.BlockSpec((local, depth), lambda b: (0, 0)),
        compiler_params=pltpu.CompilerParams(dimension_semantics=("arbitrary",), vmem_limit_bytes=58 * 1024 * 1024),
        cost_estimate=pl.CostEstimate(flops=2 * tiles * tokens * local * depth, bytes_accessed=2 * (feats_local.size + grad.size) + 4 * local * depth, transcendentals=0),
    )(feats_local, grad)


def local_step(hidden, inter_feats, proj_grad, w_query, w_key, w_value, w_out, ln_params, gate_params, w_fc1, b_fc1, w_fc2, b_fc2, w_proj, b_proj):
    tile_count, tokens, width = hidden.shape
    real_rows = proj_grad.shape[1]
    feats = inter_feats.shape[2]
    feat_local, _ = w_proj.shape
    local_heads, head_dim = w_query.shape[1:]
    local_width = local_heads * head_dim
    group = lax.axis_size('tp')
    mine = lax.axis_index('tp')
    piece = math.gcd(feat_local, width)
    per_dev, per_feat = feat_local // piece, width // piece

    flip = lambda w: w.reshape(width, local_width).T
    w_attn = lax.all_gather(jnp.stack([flip(w_query), flip(w_key), flip(w_value), w_out.reshape(local_width, width)]), 'tp', axis=1, tiled=True)
    w_mlp = lax.all_gather(jnp.stack([w_fc1.T, w_fc2]), 'tp', axis=1, tiled=True)
    fc1, fc2 = w_mlp[0], w_mlp[1]
    bias1 = lax.all_gather(b_fc1, 'tp', axis=0, tiled=True)
    proj_grad, bias1 = after(proj_grad, bias1)
    gather_rows = lambda part: lax.all_gather(part, 'tp', axis=0, tiled=True)
    w_parts = [w_proj[j * piece:(j + 1) * piece] for j in range(per_dev)]

    x_wide = lax.dynamic_index_in_dim(hidden, mine, 0, keepdims=False).astype(jnp.float32)
    normed, norm1_pull = jax.vjp(layer_norm, x_wide, ln_params[0], ln_params[1])
    proj_grad = with_layout_constraint(proj_grad, Layout((0, 1, 2)))
    normed, (proj_grad, w_parts[0]) = after(normed, (proj_grad, w_parts[0]))
    proj_rows = [gather_rows(w_parts[0])]
    qkv = matmul('td,jd->tj', normed, w_attn.reshape(-1, width)).astype(jnp.bfloat16)
    context = attend(real_rows, head_dim, width, qkv)
    attn_out = matmul('tj,jd->td', context, w_attn[3])
    gate_attn = jnp.tanh(gate_params[0])
    gate_mlp = jnp.tanh(gate_params[1])
    x_one_wide = (x_wide + gate_attn * attn_out).astype(jnp.bfloat16).astype(jnp.float32)
    normed_two, norm2_pull = jax.vjp(layer_norm, x_one_wide, ln_params[2], ln_params[3])
    pre_act = matmul('td,fd->tf', normed_two, fc1) + bias1
    mlp_act, gelu_pull = jax.vjp(gelu_bf16, pre_act)
    mlp_out = matmul('tf,fd->td', mlp_act, fc2) + b_fc2
    x_two = (x_one_wide + gate_mlp * mlp_out).astype(jnp.bfloat16)

    inter = jnp.transpose(inter_feats, (0, 2, 1, 3))
    grad_mine = lax.dynamic_index_in_dim(proj_grad, mine, 0, keepdims=False)

    def feats_part(j, prior):
        blocks = []
        for d in range(group):
            at = d * per_dev + j
            if at >= per_feat:
                blocks.append((d, at // per_feat - 1, at % per_feat))
        return grad_feats_part(proj_grad, proj_rows[j], tuple(blocks), piece, feats, tokens, width, prior)

    w_parts[1], w_attn = after(w_parts[1], w_attn)
    proj_rows.append(gather_rows(w_parts[1]))
    proj_rows[0], x_two = after(proj_rows[0], x_two)
    for part in w_parts[2:]:
        part, proj_rows[0] = after(part, proj_rows[0])
        proj_rows.append(gather_rows(part))
    grad_inter = feats_part(0, None)
    for j in range(1, per_dev - 1):
        proj_rows[j], grad_inter = after(proj_rows[j], grad_inter)
        grad_inter = feats_part(j, grad_inter)
    x_two, proj_rows[-2] = after(x_two, proj_rows[-2])
    x_two_all = lax.all_gather(x_two, 'tp', axis=0, tiled=False)
    proj_rows[-1], grad_inter = after(proj_rows[-1], grad_inter)

    rows_two = jnp.concatenate([proj_rows[at % per_dev][(at // per_dev) * piece:(at // per_dev + 1) * piece] for at in range(per_feat)], axis=0)
    grad_x_two = matmul('tp,cp->tc', grad_mine, rows_two).astype(jnp.bfloat16)
    grad_x_two = jnp.pad(grad_x_two, ((0, tokens - real_rows), (0, 0))).astype(jnp.float32)
    grad_mlp = gate_mlp * grad_x_two
    grad_gate_mlp = jnp.sum(grad_x_two * mlp_out) * (1.0 - gate_mlp * gate_mlp)
    grad_b_fc2 = jnp.sum(grad_mlp, axis=0)
    grad_mlp_low = grad_mlp.astype(jnp.bfloat16)
    grad_fc2 = matmul('tf,td->fd', mlp_act, grad_mlp_low).astype(jnp.bfloat16)
    grad_act = matmul('td,fd->tf', grad_mlp_low, fc2).astype(jnp.bfloat16)
    grad_pre = gelu_pull(grad_act)[0]
    grad_b_fc1 = jnp.sum(grad_pre, axis=0)
    grad_pre_low = grad_pre.astype(jnp.bfloat16)
    grad_fc1 = matmul('tf,td->fd', grad_pre_low, normed_two).astype(jnp.bfloat16)
    grad_normed_two = matmul('tf,fd->td', grad_pre_low, fc1).astype(jnp.bfloat16)
    grad_normed_two, (grad_fc1, grad_fc2) = after(grad_normed_two, (grad_fc1, grad_fc2))
    grad_w_fc2 = lax.psum_scatter(grad_fc2, 'tp', scatter_dimension=0, tiled=True)
    grad_w_fc1 = lax.psum_scatter(grad_fc1, 'tp', scatter_dimension=0, tiled=True)
    grad_x_ln_two, grad_gain_two, grad_bias_two = norm2_pull(grad_normed_two)
    grad_x_one = (grad_x_two + grad_x_ln_two).astype(jnp.bfloat16).astype(jnp.float32)
    grad_attn = gate_attn * grad_x_one
    grad_gate_attn = jnp.sum(grad_x_one * attn_out) * (1.0 - gate_attn * gate_attn)
    grad_attn_low = grad_attn.astype(jnp.bfloat16)
    grad_wo = matmul('tj,td->jd', context, grad_attn_low)
    grad_context = matmul('td,jd->tj', grad_attn_low, w_attn[3]).astype(jnp.bfloat16)
    grad_qkv = attend(real_rows, head_dim, width, qkv, grad_context)
    grad_wqkv = matmul('gtj,td->gjd', grad_qkv, normed)
    grad_w_attn = jnp.concatenate([grad_wqkv, grad_wo[None]]).astype(jnp.bfloat16)
    grad_w_attn = lax.psum_scatter(grad_w_attn, 'tp', scatter_dimension=1, tiled=True).astype(jnp.float32)
    unflip = lambda g: g.T.reshape(width, local_heads, head_dim)
    grad_normed = matmul('gtj,gjd->td', grad_qkv, w_attn[:3]).astype(jnp.bfloat16)
    grad_x_ln, grad_gain, grad_bias = norm1_pull(grad_normed)
    grad_tile = (grad_x_one + grad_x_ln).astype(jnp.bfloat16)

    x_two_all, grad_tile = after(x_two_all, grad_tile)
    cols = []
    for j in range(per_dev):
        at = mine * per_dev + j
        feat, col = at // per_feat, (at % per_feat) * piece
        from_two = lax.dynamic_slice_in_dim(x_two_all, col, piece, axis=2)
        from_inter = lax.dynamic_slice(inter, (0, jnp.maximum(feat - 1, 0), 0, col), (tile_count, 1, tokens, piece))[:, 0]
        cols.append(jnp.where(feat == 0, from_two, from_inter))
    grad_w_proj = rows_grad(jnp.concatenate(cols, axis=-1), proj_grad)

    grad_b_proj = jnp.sum(grad_mine, axis=0, dtype=jnp.float32)
    small = [grad_gain, grad_bias, grad_gain_two, grad_bias_two, grad_b_fc2, grad_b_fc1, grad_b_proj, jnp.stack([grad_gate_attn, grad_gate_mlp])]
    lines = [-(-v.shape[0] // width) for v in small]
    ends = [sum(lines[:n + 1]) for n in range(len(small))]
    total = -(-ends[-1] // 8) * 8
    small = jnp.concatenate([jnp.pad(v, (0, n * width - v.shape[0])).reshape(n, width) for v, n in zip(small, lines)])
    terms = split_exact(jnp.pad(small, ((0, total - ends[-1]), (0, 0)))).reshape(3 * total, width)
    grad_tile, (grad_w_fc1, grad_w_fc2) = after(grad_tile, (grad_w_fc1, grad_w_fc2))
    grad_tile, grad_w_proj = after(grad_tile, grad_w_proj)
    gathered = lax.all_gather(jnp.concatenate([grad_tile, terms]), 'tp', axis=0, tiled=False)
    grad_hidden = gathered[:, :tokens]
    sums = jnp.sum(gathered[:, tokens:].reshape(group * 3, total, width).astype(jnp.float32), axis=0)
    grad_ln, grad_b_fc2 = sums[:4], sums[4]
    grad_b_fc1 = lax.dynamic_slice_in_dim(sums[ends[4]:ends[5]].reshape(-1), mine * b_fc1.shape[0], b_fc1.shape[0], axis=0)
    grad_b_proj = sums[ends[5]:ends[6]].reshape(-1)[:b_proj.shape[0]]
    grad_gates = sums[ends[6], :2]
    grad_w_fc1, grad_w_fc2 = grad_w_fc1.astype(jnp.float32).T, grad_w_fc2.astype(jnp.float32)

    proj_rows[-1], grad_tile = after(proj_rows[-1], grad_tile)
    grad_inter = jnp.transpose(feats_part(per_dev - 1, grad_inter), (0, 2, 1, 3))
    inter_mine = lax.dynamic_index_in_dim(inter, mine, 0, keepdims=False)
    feats_mine = jnp.concatenate([x_two[None], inter_mine], axis=0)[:, :real_rows]
    proj_sum = b_proj
    for j in range(per_dev):
        part = jnp.concatenate([feats_mine[at // per_feat, :, (at % per_feat) * piece:(at % per_feat + 1) * piece]
                                for at in range(j, group * per_dev, per_dev)], axis=-1)
        proj_sum = proj_sum + matmul('tc,cp->tp', part, proj_rows[j])
    proj_out = proj_sum.astype(jnp.bfloat16)[None]
    return (proj_out, grad_hidden, grad_inter, unflip(grad_w_attn[0]), unflip(grad_w_attn[1]), unflip(grad_w_attn[2]), grad_w_attn[3].reshape(local_heads, head_dim, width), grad_ln, grad_gates, grad_w_fc1, grad_b_fc1, grad_w_fc2, grad_b_fc2, grad_w_proj, grad_b_proj)


def solution(mesh):
    tiles_spec = P('dp', None, None)
    inter_spec = P('dp', None, None, None)
    head_cols = P(None, 'tp', None)
    in_specs = (tiles_spec, inter_spec, tiles_spec, head_cols, head_cols, head_cols, P('tp', None, None), P(None, None), P(None), P(None, 'tp'), P('tp'), P('tp', None), P(None), P('tp', None), P(None))
    grad_heads = P('dp', 'tp', None)
    out_specs = (P(('dp', 'tp'), None, None), tiles_spec, inter_spec, grad_heads, grad_heads, grad_heads, P(('dp', 'tp'), None, None), P('dp', None), P('dp'), P('dp', 'tp'), P(('dp', 'tp')), P(('dp', 'tp'), None), P('dp'), P(('dp', 'tp'), None), P('dp'))

    return jax.shard_map(local_step, mesh=mesh, in_specs=in_specs, out_specs=out_specs, check_vma=False)
```

```python
import functools
import math
import jax
import jax.numpy as jnp
from jax import lax
from jax.experimental import pallas as pl
from jax.experimental.layout import Layout, with_layout_constraint
from jax.experimental.pallas import tpu as pltpu
from jax.sharding import PartitionSpec as P

LN_EPS = 1e-5


def layer_norm(values, ln_gain, ln_bias):
    row_mean = jnp.mean(values, axis=-1, keepdims=True)
    centred = values - row_mean
    row_var = jnp.mean(centred * centred, axis=-1, keepdims=True)
    return (centred * lax.rsqrt(row_var + LN_EPS) * ln_gain + ln_bias).astype(jnp.bfloat16)


def gelu_bf16(pre_act):
    return jax.nn.gelu(pre_act, approximate=False).astype(jnp.bfloat16)


def matmul(eq_form, lhs_in, rhs_in):
    return jnp.einsum(eq_form, lhs_in, rhs_in, preferred_element_type=jnp.float32)


def after(value, earlier):
    return lax.optimization_barrier((value, earlier))


def head_probs(real_rows, q_act, k_pad):
    scores = lax.dot_general(q_act, k_pad, (((1,), (1,)), ((), ())), preferred_element_type=jnp.float32)
    key_ok = lax.broadcasted_iota(jnp.int32, scores.shape, 1) < real_rows
    scores = jnp.where(key_ok, scores * q_act.shape[1] ** -0.5, -1e30)
    raised = jnp.exp(scores - jnp.max(scores, axis=-1, keepdims=True))
    return raised * (1.0 / jnp.sum(raised, axis=-1, keepdims=True))


def pad_keys(pads, refs):
    tokens = refs[0].shape[0]
    for pad_ref, ref in zip(pads, refs):
        pad_ref[0:tokens, :] = ref[...]
        pad_ref[tokens:, :] = jnp.zeros((pad_ref.shape[0] - tokens, pad_ref.shape[1]), pad_ref.dtype)


def attend_kernel(real_rows, head_dim, q_ref, k_ref, v_ref, out_ref, k_pad, v_pad):
    pad_keys((k_pad, v_pad), (k_ref, v_ref))
    for at in range(0, q_ref.shape[1], head_dim):
        cols = slice(at, at + head_dim)
        probs = head_probs(real_rows, q_ref[:, cols], k_pad[:, cols]).astype(jnp.bfloat16)
        out_ref[:, cols] = jnp.dot(probs, v_pad[:, cols], preferred_element_type=jnp.float32).astype(jnp.bfloat16)


def attend_grad_kernel(real_rows, head_dim, q_ref, k_ref, v_ref, grad_ref, out_ref, k_pad, v_pad):
    pad_keys((k_pad, v_pad), (k_ref, v_ref))
    tokens = q_ref.shape[0]
    over_rows = (((0,), (0,)), ((), ()))
    for at in range(0, q_ref.shape[1], head_dim):
        cols = slice(at, at + head_dim)
        q_act, grad = q_ref[:, cols], grad_ref[:, cols]
        probs = head_probs(real_rows, q_act, k_pad[:, cols])
        grad_v = lax.dot_general(probs.astype(jnp.bfloat16), grad, over_rows, preferred_element_type=jnp.float32)
        grad_p = lax.dot_general(grad, v_pad[:, cols], (((1,), (1,)), ((), ())), preferred_element_type=jnp.float32)
        grad_p = grad_p.astype(jnp.bfloat16).astype(jnp.float32)
        centre = jnp.sum(probs * grad_p, axis=-1, keepdims=True)
        grad_s = (probs * (grad_p - centre)).astype(jnp.bfloat16)
        grad_k = lax.dot_general(grad_s, q_act, over_rows, preferred_element_type=jnp.float32)
        grad_q = jnp.dot(grad_s, k_pad[:, cols], preferred_element_type=jnp.float32)
        out_ref[0, :, cols] = (grad_q * head_dim ** -0.5).astype(jnp.bfloat16)
        out_ref[1, :, cols] = (grad_k[0:tokens] * head_dim ** -0.5).astype(jnp.bfloat16)
        out_ref[2, :, cols] = grad_v[0:tokens].astype(jnp.bfloat16)


def attend(real_rows, head_dim, width, qkv, grad=None):
    tokens = qkv.shape[0]
    lanes = max(128, head_dim)
    steps = width // lanes
    keys = (tokens + 127) // 128 * 128
    part = lambda n: pl.BlockSpec((tokens, lanes), lambda h, n=n: (0, n * steps + h))
    one = 2 * tokens * keys * width
    args, in_specs = [qkv, qkv, qkv], [part(0), part(1), part(2)]
    if grad is None:
        kernel, dots = attend_kernel, 2
        out_shape, out_specs = (tokens, width), part(0)
    else:
        kernel, dots = attend_grad_kernel, 5
        args, in_specs = args + [grad], in_specs + [part(0)]
        out_shape, out_specs = (3, tokens, width), pl.BlockSpec((3, tokens, lanes), lambda h: (0, 0, h))
    return pl.pallas_call(
        functools.partial(kernel, real_rows, head_dim),
        grid=(steps,),
        out_shape=jax.ShapeDtypeStruct(out_shape, jnp.bfloat16),
        in_specs=in_specs,
        out_specs=out_specs,
        scratch_shapes=[pltpu.VMEM((keys, lanes), jnp.bfloat16)] * 2,
        compiler_params=pltpu.CompilerParams(dimension_semantics=("arbitrary",), vmem_limit_bytes=40 * 1024 * 1024),
        cost_estimate=pl.CostEstimate(flops=4 * dots * one, bytes_accessed=16 * tokens * width, transcendentals=0),
    )(*args)


def split_exact(values):
    high = lax.reduce_precision(values, 8, 7)
    mid = lax.reduce_precision(values - high, 8, 7)
    return jnp.stack([high, mid, values - high - mid]).astype(jnp.bfloat16)


def feats_kernel(blocks, piece, real_rows, grad_ref, rows_ref, *rest):
    out_ref, held, sems = rest[-3:]
    tokens = held.shape[2]
    tile = pl.program_id(0)
    tiles = pl.num_programs(0)
    slot = lax.rem(tile, 2)

    def copies(at_tile, at_slot):
        return [pltpu.make_async_copy(held.at[at_slot, n],
                                      out_ref.at[at_tile, feat, :, pl.ds(col * piece, piece)],
                                      sems.at[at_slot, n])
                for n, (_, feat, col) in enumerate(blocks)]

    @pl.when(tile >= 2)
    def _():
        for copy in copies(tile - 2, slot):
            copy.wait()

    is_real = lax.broadcasted_iota(jnp.int32, (tokens, piece), 0) < real_rows
    out_now = copies(tile, slot)
    for n, (row, _, _) in enumerate(blocks):
        block = lax.dot_general(grad_ref[0], rows_ref[pl.ds(row * piece, piece), :],
                                (((1,), (1,)), ((), ())), preferred_element_type=jnp.float32)
        held[slot, n] = jnp.where(is_real, block, 0.0).astype(jnp.bfloat16)
        out_now[n].start()

    @pl.when(tile == tiles - 1)
    def _():
        for copy in copies(tile - 1, 1 - slot) + out_now:
            copy.wait()


def grad_feats_part(grad, rows, blocks, piece, feats, tokens, width, prior):
    tiles, real_rows, depth = grad.shape
    flops = 2 * tiles * tokens * depth * piece * len(blocks)
    in_specs = [pl.BlockSpec((1, tokens, depth), lambda b: (b, 0, 0)),
                pl.BlockSpec(rows.shape, lambda b: (0, 0), pipeline_mode=pl.Buffered(1))]
    args = [grad, rows]
    aliases = {}
    if prior is not None:
        in_specs.append(pl.BlockSpec(memory_space=pl.ANY))
        args.append(prior)
        aliases = {2: 0}
    return pl.pallas_call(
        functools.partial(feats_kernel, blocks, piece, real_rows),
        grid=(tiles,),
        out_shape=jax.ShapeDtypeStruct((tiles, feats, tokens, width), jnp.bfloat16),
        in_specs=in_specs,
        out_specs=pl.BlockSpec(memory_space=pl.ANY),
        scratch_shapes=[pltpu.VMEM((2, len(blocks), tokens, piece), jnp.bfloat16),
                        pltpu.SemaphoreType.DMA((2, len(blocks)))],
        input_output_aliases=aliases,
        compiler_params=pltpu.CompilerParams(dimension_semantics=("arbitrary",), vmem_limit_bytes=58 * 1024 * 1024),
        cost_estimate=pl.CostEstimate(flops=flops, bytes_accessed=2 * (grad.size + rows.size + tiles * tokens * piece * len(blocks)), transcendentals=0),
    )(*args)


def rows_grad_kernel(real_rows, step, feats_ref, grad_ref, out_ref):
    tile = pl.program_id(0)
    pair, tokens, depth = grad_ref.shape

    @pl.when(tile == 0)
    def _():
        out_ref[...] = jnp.zeros_like(out_ref)

    is_real = lax.broadcasted_iota(jnp.int32, (pair, tokens, step), 1) < real_rows
    turned = feats_ref[...].reshape(pair * tokens, -1).T
    for at in range(0, depth, step):
        cols = pl.ds(at, step)
        grad = jnp.where(is_real, grad_ref[:, :, cols], jnp.bfloat16(0)).reshape(pair * tokens, step)
        out_ref[:, cols] += jnp.dot(turned, grad, preferred_element_type=jnp.float32)


def rows_grad(feats_local, grad):
    tiles, tokens, local = feats_local.shape
    real_rows, depth = grad.shape[1:]
    pair = 2 - tiles % 2
    return pl.pallas_call(
        functools.partial(rows_grad_kernel, real_rows, min(512, depth)),
        grid=(tiles // pair,),
        out_shape=jax.ShapeDtypeStruct((local, depth), jnp.float32),
        in_specs=[pl.BlockSpec((pair, tokens, local), lambda b: (b, 0, 0)),
                  pl.BlockSpec((pair, tokens, depth), lambda b: (b, 0, 0))],
        out_specs=pl.BlockSpec((local, depth), lambda b: (0, 0)),
        compiler_params=pltpu.CompilerParams(dimension_semantics=("arbitrary",), vmem_limit_bytes=58 * 1024 * 1024),
        cost_estimate=pl.CostEstimate(flops=2 * tiles * tokens * local * depth, bytes_accessed=2 * (feats_local.size + grad.size) + 4 * local * depth, transcendentals=0),
    )(feats_local, grad)


def local_step(hidden, inter_feats, proj_grad, w_query, w_key, w_value, w_out, ln_params, gate_params, w_fc1, b_fc1, w_fc2, b_fc2, w_proj, b_proj):
    tile_count, tokens, width = hidden.shape
    real_rows = proj_grad.shape[1]
    feats = inter_feats.shape[2]
    feat_local, _ = w_proj.shape
    local_heads, head_dim = w_query.shape[1:]
    local_width = local_heads * head_dim
    group = lax.axis_size('tp')
    mine = lax.axis_index('tp')
    piece = math.gcd(feat_local, width)
    per_dev, per_feat = feat_local // piece, width // piece

    flip = lambda w: w.reshape(width, local_width).T
    w_attn = lax.all_gather(jnp.stack([flip(w_query), flip(w_key), flip(w_value), w_out.reshape(local_width, width)]), 'tp', axis=1, tiled=True)
    mlp_part = jnp.stack([w_fc1.T, w_fc2])
    bias1 = lax.all_gather(b_fc1, 'tp', axis=0, tiled=True)
    proj_grad, bias1 = after(proj_grad, bias1)
    gather_rows = lambda part: lax.all_gather(part, 'tp', axis=0, tiled=True)
    w_parts = [w_proj[j * piece:(j + 1) * piece] for j in range(per_dev)]

    x_wide = lax.dynamic_index_in_dim(hidden, mine, 0, keepdims=False).astype(jnp.float32)
    normed, norm1_pull = jax.vjp(layer_norm, x_wide, ln_params[0], ln_params[1])
    proj_grad = with_layout_constraint(proj_grad, Layout((0, 1, 2)))
    normed, proj_grad = after(normed, proj_grad)
    proj_rows = [gather_rows(w_parts[0])]
    w_mlp = lax.all_gather(mlp_part, 'tp', axis=1, tiled=True)
    qkv = matmul('td,jd->tj', normed, w_attn.reshape(-1, width)).astype(jnp.bfloat16)
    context = attend(real_rows, head_dim, width, qkv)
    w_parts[1], context = after(w_parts[1], context)
    proj_rows.append(gather_rows(w_parts[1]))
    attn_out = matmul('tj,jd->td', context, w_attn[3])
    gate_attn = jnp.tanh(gate_params[0])
    gate_mlp = jnp.tanh(gate_params[1])
    x_one_wide = (x_wide + gate_attn * attn_out).astype(jnp.bfloat16).astype(jnp.float32)
    normed_two, norm2_pull = jax.vjp(layer_norm, x_one_wide, ln_params[2], ln_params[3])
    inter = jnp.transpose(inter_feats, (0, 2, 1, 3))
    grad_mine = lax.dynamic_index_in_dim(proj_grad, mine, 0, keepdims=False)

    def feats_part(j, prior):
        blocks = []
        for d in range(group):
            at = d * per_dev + j
            if at >= per_feat:
                blocks.append((d, at // per_feat - 1, at % per_feat))
        return grad_feats_part(proj_grad, proj_rows[j], tuple(blocks), piece, feats, tokens, width, prior)

    grad_inter = feats_part(0, None)
    w_mlp, grad_inter = after(w_mlp, grad_inter)
    fc1, fc2 = w_mlp[0], w_mlp[1]
    pre_act = matmul('td,fd->tf', normed_two, fc1) + bias1
    mlp_act, gelu_pull = jax.vjp(gelu_bf16, pre_act)
    mlp_out = matmul('tf,fd->td', mlp_act, fc2) + b_fc2
    x_two = (x_one_wide + gate_mlp * mlp_out).astype(jnp.bfloat16)

    for part in w_parts[2:]:
        part, x_two = after(part, x_two)
        proj_rows.append(gather_rows(part))
    inter_mine = lax.dynamic_index_in_dim(inter, mine, 0, keepdims=False)
    feats_mine = jnp.concatenate([x_two[None], inter_mine], axis=0)[:, :real_rows]

    def proj_term(j):
        part = jnp.concatenate([feats_mine[at // per_feat, :, (at % per_feat) * piece:(at % per_feat + 1) * piece]
                                for at in range(j, group * per_dev, per_dev)], axis=-1)
        return matmul('tc,cp->tp', part, proj_rows[j])

    proj_sum = b_proj + proj_term(0)
    grad_b_proj = jnp.sum(grad_mine, axis=0, dtype=jnp.float32)
    proj_rows[1], (proj_sum, grad_b_proj) = after(proj_rows[1], (proj_sum, grad_b_proj))
    for j in range(1, per_dev - 1):
        proj_rows[j], grad_inter = after(proj_rows[j], grad_inter)
        grad_inter = feats_part(j, grad_inter)
    x_two, proj_rows[-2] = after(x_two, proj_rows[-2])
    x_two_all = lax.all_gather(x_two, 'tp', axis=0, tiled=False)
    proj_rows[-1], grad_inter = after(proj_rows[-1], grad_inter)

    rows_two = jnp.concatenate([proj_rows[at % per_dev][(at // per_dev) * piece:(at // per_dev + 1) * piece] for at in range(per_feat)], axis=0)
    grad_x_two = matmul('tp,cp->tc', grad_mine, rows_two).astype(jnp.bfloat16)
    grad_x_two = jnp.pad(grad_x_two, ((0, tokens - real_rows), (0, 0))).astype(jnp.float32)
    grad_mlp = gate_mlp * grad_x_two
    grad_gate_mlp = jnp.sum(grad_x_two * mlp_out) * (1.0 - gate_mlp * gate_mlp)
    grad_b_fc2 = jnp.sum(grad_mlp, axis=0)
    grad_mlp_low = grad_mlp.astype(jnp.bfloat16)
    grad_fc2 = matmul('tf,td->fd', mlp_act, grad_mlp_low).astype(jnp.bfloat16)
    grad_act = matmul('td,fd->tf', grad_mlp_low, fc2).astype(jnp.bfloat16)
    grad_pre = gelu_pull(grad_act)[0]
    grad_b_fc1 = jnp.sum(grad_pre, axis=0)
    grad_pre_low = grad_pre.astype(jnp.bfloat16)
    grad_fc1 = matmul('tf,td->fd', grad_pre_low, normed_two).astype(jnp.bfloat16)
    grad_normed_two = matmul('tf,fd->td', grad_pre_low, fc1).astype(jnp.bfloat16)
    grad_normed_two, (grad_fc1, grad_fc2) = after(grad_normed_two, (grad_fc1, grad_fc2))
    grad_w_fc2 = lax.psum_scatter(grad_fc2, 'tp', scatter_dimension=0, tiled=True)
    grad_w_fc1 = lax.psum_scatter(grad_fc1, 'tp', scatter_dimension=0, tiled=True)
    grad_x_ln_two, grad_gain_two, grad_bias_two = norm2_pull(grad_normed_two)
    grad_x_one = (grad_x_two + grad_x_ln_two).astype(jnp.bfloat16).astype(jnp.float32)
    grad_attn = gate_attn * grad_x_one
    grad_gate_attn = jnp.sum(grad_x_one * attn_out) * (1.0 - gate_attn * gate_attn)
    grad_attn_low = grad_attn.astype(jnp.bfloat16)
    grad_wo = matmul('tj,td->jd', context, grad_attn_low)
    grad_context = matmul('td,jd->tj', grad_attn_low, w_attn[3]).astype(jnp.bfloat16)
    grad_qkv = attend(real_rows, head_dim, width, qkv, grad_context)
    grad_wqkv = matmul('gtj,td->gjd', grad_qkv, normed)
    grad_w_attn = jnp.concatenate([grad_wqkv, grad_wo[None]]).astype(jnp.bfloat16)
    grad_w_attn = lax.psum_scatter(grad_w_attn, 'tp', scatter_dimension=1, tiled=True).astype(jnp.float32)
    unflip = lambda g: g.T.reshape(width, local_heads, head_dim)
    grad_normed = matmul('gtj,gjd->td', grad_qkv, w_attn[:3]).astype(jnp.bfloat16)
    grad_x_ln, grad_gain, grad_bias = norm1_pull(grad_normed)
    grad_tile = (grad_x_one + grad_x_ln).astype(jnp.bfloat16)

    x_two_all, grad_tile = after(x_two_all, grad_tile)
    cols = []
    for j in range(per_dev):
        at = mine * per_dev + j
        feat, col = at // per_feat, (at % per_feat) * piece
        from_two = lax.dynamic_slice_in_dim(x_two_all, col, piece, axis=2)
        from_inter = lax.dynamic_slice(inter, (0, jnp.maximum(feat - 1, 0), 0, col), (tile_count, 1, tokens, piece))[:, 0]
        cols.append(jnp.where(feat == 0, from_two, from_inter))
    grad_w_proj = rows_grad(jnp.concatenate(cols, axis=-1), proj_grad)

    small = [grad_gain, grad_bias, grad_gain_two, grad_bias_two, grad_b_fc2, grad_b_fc1, grad_b_proj, jnp.stack([grad_gate_attn, grad_gate_mlp])]
    lines = [-(-v.shape[0] // width) for v in small]
    ends = [sum(lines[:n + 1]) for n in range(len(small))]
    total = -(-ends[-1] // 8) * 8
    small = jnp.concatenate([jnp.pad(v, (0, n * width - v.shape[0])).reshape(n, width) for v, n in zip(small, lines)])
    terms = split_exact(jnp.pad(small, ((0, total - ends[-1]), (0, 0)))).reshape(3 * total, width)
    grad_tile, (grad_w_fc1, grad_w_fc2) = after(grad_tile, (grad_w_fc1, grad_w_fc2))
    grad_tile, grad_w_proj = after(grad_tile, grad_w_proj)
    gathered = lax.all_gather(jnp.concatenate([grad_tile, terms]), 'tp', axis=0, tiled=False)
    grad_hidden = gathered[:, :tokens]
    sums = jnp.sum(gathered[:, tokens:].reshape(group * 3, total, width).astype(jnp.float32), axis=0)
    grad_ln, grad_b_fc2 = sums[:4], sums[4]
    grad_b_fc1 = lax.dynamic_slice_in_dim(sums[ends[4]:ends[5]].reshape(-1), mine * b_fc1.shape[0], b_fc1.shape[0], axis=0)
    grad_b_proj = sums[ends[5]:ends[6]].reshape(-1)[:b_proj.shape[0]]
    grad_gates = sums[ends[6], :2]
    grad_w_fc1, grad_w_fc2 = grad_w_fc1.astype(jnp.float32).T, grad_w_fc2.astype(jnp.float32)

    proj_rows[-1], grad_tile = after(proj_rows[-1], grad_tile)
    grad_inter = jnp.transpose(feats_part(per_dev - 1, grad_inter), (0, 2, 1, 3))
    for j in range(1, per_dev):
        proj_sum = proj_sum + proj_term(j)
    proj_out = proj_sum.astype(jnp.bfloat16)[None]
    return (proj_out, grad_hidden, grad_inter, unflip(grad_w_attn[0]), unflip(grad_w_attn[1]), unflip(grad_w_attn[2]), grad_w_attn[3].reshape(local_heads, head_dim, width), grad_ln, grad_gates, grad_w_fc1, grad_b_fc1, grad_w_fc2, grad_b_fc2, grad_w_proj, grad_b_proj)


def solution(mesh):
    tiles_spec = P('dp', None, None)
    inter_spec = P('dp', None, None, None)
    head_cols = P(None, 'tp', None)
    in_specs = (tiles_spec, inter_spec, tiles_spec, head_cols, head_cols, head_cols, P('tp', None, None), P(None, None), P(None), P(None, 'tp'), P('tp'), P('tp', None), P(None), P('tp', None), P(None))
    grad_heads = P('dp', 'tp', None)
    out_specs = (P(('dp', 'tp'), None, None), tiles_spec, inter_spec, grad_heads, grad_heads, grad_heads, P(('dp', 'tp'), None, None), P('dp', None), P('dp'), P('dp', 'tp'), P(('dp', 'tp')), P(('dp', 'tp'), None), P('dp'), P(('dp', 'tp'), None), P('dp'))

    return jax.shard_map(local_step, mesh=mesh, in_specs=in_specs, out_specs=out_specs, check_vma=False)
```
